32 devices in a mesh: frame: 16 (over z, y, core), stream: 2 (over x).
Axes of the slice: x: 2, y: 2, z: 4, core: 2. Of those that a mesh axis runs over, the one named last changes fastest.
Arguments:
- query: bfloat16 [2, 2048, 4096], P('stream', 'frame'), may hold values from -60 to 60
- key: bfloat16 [2, 2048, 4096], P('stream', 'frame'), may hold values from -4 to 4
- value: bfloat16 [2, 2048, 4096], P('stream', 'frame'), may hold values from -24 to 24
- latent: bfloat16 [2, 2048, 4096], P('stream', 'frame'), may hold values from -6 to 6
- target: bfloat16 [2, 2048, 4096], P('stream', 'frame'), may hold values from -6 to 6
- noise_level: float32 [2, 16], P('stream'), may hold values from 0.02 to 0.98
- mod_weight: bfloat16 [4096, 256], replicated, may hold values from -0.375 to 0.375
- block_order: int32 [32], replicated, may hold values from 0 to 31, as said below
- context_start: int32 [2, 16], P('stream'), may hold values from 0 to 15, as said below
Outputs:
- grad_weight: float32 [4096, 256], P('frame')
The draws below stay inside these ranges and needn't reach their ends.
Inputs may be any that keep to these rules, and one draw needn't show every extreme that they name: block_order is a permutation of 0 to 31, and entries 2 i and 2 i + 1 add up to 31. context_start[s, c] lies between 0 and c.
All inputs are finite; a program needn't handle non-finite values.
Results may differ from the reference program's by a relative error of at most 0.0016.
Values may be sent and summed in bfloat16 or wider, within the bound.
A program may use at most 64 MiB of HBM per device.

```python
import math
import jax
import jax.numpy as jnp
from jax import lax

HEAD_DIM = 128
HEADS = 32
D = 4096
FREQ = 256
GROUPS = 16
BLOCK_LEN = 64
BLOCKS = 32
SEQ = 2048
GROUP_LEN = 128
STREAMS = 2
N_FRAME = 16


def drawn_pair(key):
    shape = (STREAMS, SEQ, D)
    keys = jnp.clip(jax.random.normal(jax.random.fold_in(key, 101), shape, jnp.float32), -4.0, 4.0)
    queries = jnp.clip(jax.random.normal(jax.random.fold_in(key, 202), shape, jnp.float32), -4.0, 4.0)
    return (queries, keys)


def draw_query(key, part):
    pair = drawn_pair(key)
    return pair[0].astype(jnp.bfloat16)


def draw_key(key, part):
    pair = drawn_pair(key)
    return pair[1].astype(jnp.bfloat16)


def draw_block_order(key, part):
    order = jax.random.permutation(jax.random.fold_in(key, 11), N_FRAME).astype(jnp.int32)
    flipped = jax.random.randint(jax.random.fold_in(key, 12), (N_FRAME,), 0, 2)
    first = jnp.where(flipped == 1, BLOCKS - 1 - order, order)
    second = BLOCKS - 1 - first
    return jnp.stack([first, second], axis=1).reshape(BLOCKS).astype(jnp.int32)


def draw_context_start(key, part):
    upper = jnp.arange(GROUPS, dtype=jnp.int32)[None, :] + 1
    return jax.random.randint(jax.random.fold_in(key, 21), (STREAMS, GROUPS), 0, upper).astype(jnp.int32)


def steps_of(own_key, extent, split, low, top_value):
    level = 1.0
    for axis_at, shards_of in split:
        draws = jax.random.uniform(jax.random.fold_in(jax.random.fold_in(own_key, 6), axis_at), (shards_of,), jnp.float32, low / len(split), top_value / len(split))
        level = level * jnp.repeat(jnp.exp(draws), extent[axis_at] // shards_of).reshape((-1,) + (1,) * (len(extent) - 1 - axis_at))
    return level


def normal_values(rng, dims, spread, bound, split=(), kind=jnp.bfloat16):
    result = jax.random.normal(rng, dims, jnp.float32) * spread
    if len(split) > 0:
        result = steps_of(rng, dims, split, -0.22, 0.18) * result
    return jnp.clip(result, min=-bound, max=bound).astype(kind)


def setup_inputs(seed: int = 0) -> dict:
    streams_of = jax.random.split(jax.random.key(seed), 10)
    return {
        "query": draw_query(jax.random.fold_in(streams_of[9], 71), 0),
        "key": draw_key(jax.random.fold_in(streams_of[9], 71), 0),
        "value": normal_values(streams_of[2], (STREAMS, SEQ, D), 4.0, 24.0, ((0, 2), (1, 16))),
        "latent": normal_values(streams_of[3], (STREAMS, SEQ, D), 1.0, 6.0, ((0, 2), (1, 16))),
        "target": normal_values(streams_of[4], (STREAMS, SEQ, D), 1.0, 6.0, ((0, 2), (1, 16))),
        "noise_level": jnp.clip(0.02 + 0.96000002 * jax.random.uniform(streams_of[5], (STREAMS, GROUPS), jnp.float32) ** steps_of(streams_of[5], (STREAMS, GROUPS), ((0, 2),), -0.2, 0.2), 0.02, 0.98),
        "mod_weight": normal_values(streams_of[6], (D, FREQ), FREQ ** -0.5, 0.375),
        "block_order": draw_block_order(jax.random.fold_in(streams_of[9], 71), 0),
        "context_start": draw_context_start(jax.random.fold_in(streams_of[9], 71), 0),
    }


def reference(query, key, value, latent, target, noise_level, mod_weight, block_order, context_start):
    half_width = FREQ // 2
    frequency = jnp.exp(-math.log(10000.0) * jnp.arange(half_width, dtype=jnp.float32) / half_width)
    angles = 1000.0 * noise_level[..., None] * frequency
    embed = jnp.concatenate([jnp.cos(angles), jnp.sin(angles)], -1).astype(jnp.bfloat16)
    gate = jnp.dot(embed.reshape(STREAMS * GROUPS, FREQ), mod_weight.T, preferred_element_type=jnp.float32)
    gate = gate.reshape(STREAMS, GROUPS, D)
    block_group = (block_order // (BLOCKS // GROUPS)).astype(jnp.int32)
    row_group = block_group[jnp.arange(SEQ, dtype=jnp.int32) // BLOCK_LEN]
    scale = 1.0 / math.sqrt(HEAD_DIM)

    def one_stream(stream):
        row_start = context_start[stream][row_group]
        visible = (row_start[:, None] <= row_group[None, :]) & (row_group[None, :] <= row_group[:, None])
        queries = query[stream].reshape(SEQ, HEADS, HEAD_DIM).transpose(1, 0, 2)
        keys = key[stream].reshape(SEQ, HEADS, HEAD_DIM).transpose(1, 0, 2)
        values = value[stream].reshape(SEQ, HEADS, HEAD_DIM).transpose(1, 0, 2)

        def one_head(parts):
            scores = jnp.dot(parts[0], parts[1].T, preferred_element_type=jnp.float32) * scale
            masked = jnp.where(visible, scores, -jnp.inf)
            peak = lax.optimization_barrier(jnp.max(masked, axis=-1, keepdims=True))
            unnorm = jnp.where(visible, jnp.exp(masked - peak), 0.0)
            probs = (unnorm / lax.optimization_barrier(jnp.sum(unnorm, axis=-1, keepdims=True))).astype(jnp.bfloat16)
            return jnp.dot(probs, parts[2], preferred_element_type=jnp.float32).astype(jnp.bfloat16)
        heads_out = lax.map(one_head, (queries, keys, values))
        attn_wide = heads_out.transpose(1, 0, 2).reshape(SEQ, D).astype(jnp.float32)
        error = latent[stream].astype(jnp.float32) + gate[stream][row_group] * attn_wide - target[stream].astype(jnp.float32)
        return jax.ops.segment_sum(attn_wide * error, row_group, num_segments=GROUPS)
    group_sum = lax.map(one_stream, jnp.arange(STREAMS, dtype=jnp.int32))
    grad_weight = jnp.dot(group_sum.reshape(STREAMS * GROUPS, D).T, embed.astype(jnp.float32).reshape(STREAMS * GROUPS, FREQ), precision=lax.Precision.HIGHEST)
    return grad_weight / math.sqrt(GROUP_LEN)
```

```python
import functools
import math

import jax
import jax.numpy as jnp
from jax import lax
from jax.experimental import pallas as pl
from jax.experimental.pallas import tpu as pltpu
from jax.sharding import PartitionSpec as P

HEAD_DIM = 128
HIDDEN = -1e30


def sinusoid(noise, emb_width):
    half_width = emb_width // 2
    frequency = jnp.exp(-math.log(10000.0) * jnp.arange(half_width, dtype=jnp.float32) / half_width)
    angles = 1000.0 * noise[..., None] * frequency
    return jnp.concatenate([jnp.cos(angles), jnp.sin(angles)], -1).astype(jnp.bfloat16)


def kernel(
    frames,
    streams,
    order_ref,
    start_ref,
    embed_ref,
    query_ref,
    key_ref,
    value_ref,
    latent_ref,
    target_ref,
    weight_ref,
    out_ref,
    query_in,
    key_in,
    value_in,
    diff_in,
    key_sorted,
    value_sorted,
    attn_all,
    latent_own,
    target_own,
    diff_own,
    weight_own,
    embed_all,
    sums_all,
    squares,
    place,
    send_sems,
    recv_sems,
    side_send,
    side_recv,
    local_sems,
):
    me = lax.axis_index("frame")
    my_stream = lax.axis_index("stream")
    own, block_len, width = query_ref.shape
    local = width // frames
    blocks = query_in.shape[0]
    groups = embed_ref.shape[0]
    per_group = blocks // groups
    group_len = per_group * block_len
    seq_len = blocks * block_len
    heads = local // HEAD_DIM

    def peer_of(i):
        return lax.rem(me + i // 2 + lax.rem(i, 2) * (frames // 2), frames)

    barrier = pltpu.get_barrier_semaphore()

    @pl.loop(1, frames)
    def _(i):
        pl.semaphore_signal(barrier, inc=1, device_id={"frame": peer_of(i)})

    for i in range(1, streams):
        pl.semaphore_signal(
            barrier, inc=1, device_id={"stream": lax.rem(my_stream + i, streams)}
        )

    early = (
        pltpu.make_async_copy(latent_ref, latent_own, local_sems.at[0]),
        pltpu.make_async_copy(target_ref, target_own, local_sems.at[1]),
        pltpu.make_async_copy(
            weight_ref.at[pl.ds(me * local, local), :], weight_own, local_sems.at[2]
        ),
    )
    mine = tuple(
        pltpu.make_async_copy(
            source.at[:, :, pl.ds(me * local, local)],
            landing.at[pl.ds(me * own, own)],
            local_sems.at[3 + number],
        )
        for number, (source, landing) in enumerate(
            ((key_ref, key_in), (query_ref, query_in), (value_ref, value_in))
        )
    )
    for copy in early + mine:
        copy.start()
    pl.semaphore_wait(barrier, frames - 1 + streams - 1)

    def sending(number, source, landing, peer):
        return pltpu.make_async_remote_copy(
            src_ref=source.at[:, :, pl.ds(pl.multiple_of(peer * local, local), local)],
            dst_ref=landing.at[pl.ds(me * own, own)],
            send_sem=send_sems.at[number, peer],
            recv_sem=recv_sems.at[number, me],
            device_id={"frame": peer},
        )

    def arriving(number, source, landing, peer):
        return pltpu.make_async_remote_copy(
            src_ref=source.at[:, :, pl.ds(pl.multiple_of(peer * local, local), local)],
            dst_ref=landing.at[pl.ds(peer * own, own)],
            send_sem=send_sems.at[number, peer],
            recv_sem=recv_sems.at[number, peer],
            device_id={"frame": peer},
        )

    def send_all(number, source, landing):
        @pl.loop(1, frames)
        def _(i):
            sending(number, source, landing, peer_of(i)).start()

    def await_all(number, source, landing):
        @pl.loop(1, frames)
        def _(i):
            arriving(number, source, landing, peer_of(i)).wait()

    send_all(0, key_ref, key_in)
    send_all(1, query_ref, query_in)
    send_all(2, value_ref, value_in)

    def side_copies(part, source, landing):
        return [
            pltpu.make_async_remote_copy(
                src_ref=source,
                dst_ref=landing.at[my_stream],
                send_sem=side_send.at[part, i],
                recv_sem=side_recv.at[part, i],
                device_id={"stream": lax.rem(my_stream + i, streams)},
            )
            for i in range(1, streams)
        ]

    embed_copies = side_copies(0, embed_ref, embed_all)
    for copy in embed_copies:
        copy.start()
    embed_all[my_stream] = embed_ref[...]

    for copy in early:
        copy.wait()

    @pl.loop(0, frames)
    def _(i):
        columns = pl.ds(pl.multiple_of(i * local, local), local)
        for b in range(own):
            diff_own[b, :, columns] = (
                latent_own[b, :, columns].astype(jnp.float32)
                - target_own[b, :, columns].astype(jnp.float32)
            ).astype(jnp.bfloat16)

    my_diff = pltpu.make_async_copy(
        diff_own.at[:, :, pl.ds(me * local, local)],
        diff_in.at[pl.ds(me * own, own)],
        local_sems.at[6],
    )
    send_all(3, diff_own, diff_in)
    my_diff.start()

    gate = lax.dot_general(
        embed_ref[...].astype(jnp.bfloat16),
        weight_own[...],
        (((1,), (1,)), ((), ())),
        preferred_element_type=jnp.float32,
    )

    @pl.loop(0, blocks)
    def _(t):
        found = jnp.int32(0)
        for b in range(blocks):
            found = jnp.where(order_ref[b] == t, b, found)
        place[t] = found

    for copy in mine:
        copy.wait()
    await_all(0, key_ref, key_in)

    @pl.loop(0, blocks)
    def _(t):
        rows = pl.ds(pl.multiple_of(t * block_len, block_len), block_len)
        key_sorted[rows, :] = key_in[place[t]]

    await_all(1, query_ref, query_in)
    await_all(2, value_ref, value_in)

    @pl.loop(0, blocks)
    def _(t):
        rows = pl.ds(pl.multiple_of(t * block_len, block_len), block_len)
        value_sorted[rows, :] = value_in[place[t]]

    factor = math.log2(math.e) / math.sqrt(HEAD_DIM)

    def gathered(source, c):
        return jnp.concatenate(
            [source[place[c * per_group + i]] for i in range(per_group)], axis=0
        )

    ranges = math.gcd(groups, 4)
    for number in range(ranges):
        length = (number + 1) * (seq_len // ranges)

        @pl.loop(number * (groups // ranges), (number + 1) * (groups // ranges))
        def _(c):
            rows = gathered(query_in, c)
            column_group = lax.broadcasted_iota(jnp.int32, (1, length), 1) // group_len
            bias = jnp.where(
                (column_group >= start_ref[c]) & (column_group <= c), 0.0, HIDDEN
            ).astype(jnp.float32)
            parts = []
            for h in range(heads):
                lanes = slice(h * HEAD_DIM, (h + 1) * HEAD_DIM)
                scores = (
                    lax.dot_general(
                        rows[:, lanes],
                        key_sorted[:length, lanes],
                        (((1,), (1,)), ((), ())),
                        preferred_element_type=jnp.float32,
                    )
                    + bias
                )
                peak = jnp.max(scores, axis=-1, keepdims=True)
                unnorm = jnp.exp2((scores - peak) * factor)
                inverse = 1.0 / jnp.sum(unnorm, axis=-1, keepdims=True)
                probs = (unnorm * inverse).astype(jnp.bfloat16)
                parts.append(
                    lax.dot_general(
                        probs,
                        value_sorted[:length, lanes],
                        (((1,), (0,)), ((), ())),
                        preferred_element_type=jnp.float32,
                    ).astype(jnp.bfloat16)
                )
            attn = jnp.concatenate(parts, axis=1)
            attn_all[c] = attn
            wide = attn.astype(jnp.float32)
            squares[pl.ds(c, 1), :] = jnp.sum(wide * wide, axis=0, keepdims=True)

    my_diff.wait()
    await_all(3, diff_own, diff_in)

    @pl.loop(0, groups)
    def _(c):
        product = attn_all[c].astype(jnp.float32) * gathered(diff_in, c).astype(jnp.float32)
        sums_all[my_stream, pl.ds(c, 1), :] = jnp.sum(product, axis=0, keepdims=True)

    sums_all[my_stream] = sums_all[my_stream] + gate * squares[...]
    sum_copies = side_copies(1, sums_all.at[my_stream], sums_all)
    for copy in sum_copies:
        copy.start()
    for copy in embed_copies:
        copy.wait()
    for copy in sum_copies:
        copy.wait()
    out_ref[...] = lax.dot_general(
        sums_all[...].reshape(streams * groups, local),
        embed_all[...].reshape(streams * groups, embed_ref.shape[1]),
        (((0,), (0,)), ((), ())),
        precision=lax.Precision.HIGHEST,
        preferred_element_type=jnp.float32,
    ) * (1.0 / math.sqrt(group_len))


def per_device(
    query, key, value, latent, target, noise_level, mod_weight, block_order, context_start
):
    frames = lax.axis_size("frame")
    streams = lax.axis_size("stream")
    tokens, width = query.shape[1:]
    local = width // frames
    blocks = block_order.shape[0]
    own = blocks // frames
    block_len = tokens // own
    groups = noise_level.shape[1]
    emb_width = mod_weight.shape[1]
    group_len = blocks // groups * block_len
    seq_len = blocks * block_len
    embed = sinusoid(noise_level[0], emb_width).astype(jnp.float32)
    bf16, f32 = jnp.bfloat16, jnp.float32
    shaped = [x.reshape(own, block_len, width) for x in (query, key, value, latent, target)]
    anywhere = pl.BlockSpec(memory_space=pl.ANY)
    scalars = pl.BlockSpec(memory_space=pltpu.SMEM)
    vectors = pl.BlockSpec(memory_space=pltpu.VMEM)
    landing = pltpu.VMEM((blocks, block_len, local), bf16)
    ordered = pltpu.VMEM((seq_len, local), bf16)
    held = pltpu.VMEM((own, block_len, width), bf16)
    return pl.pallas_call(
        functools.partial(kernel, frames, streams),
        out_shape=jax.ShapeDtypeStruct((local, emb_width), f32),
        in_specs=[scalars, scalars, vectors] + [anywhere] * 6,
        out_specs=vectors,
        scratch_shapes=[
            landing,
            landing,
            landing,
            landing,
            ordered,
            ordered,
            pltpu.VMEM((groups, group_len, local), bf16),
            held,
            held,
            held,
            pltpu.VMEM((local, emb_width), bf16),
            pltpu.VMEM((streams, groups, emb_width), f32),
            pltpu.VMEM((streams, groups, local), f32),
            pltpu.VMEM((groups, local), f32),
            pltpu.SMEM((blocks,), jnp.int32),
            pltpu.SemaphoreType.DMA((4, frames)),
            pltpu.SemaphoreType.DMA((4, frames)),
            pltpu.SemaphoreType.DMA((2, streams)),
            pltpu.SemaphoreType.DMA((2, streams)),
            pltpu.SemaphoreType.DMA((7,)),
        ],
        compiler_params=pltpu.CompilerParams(
            collective_id=0, has_side_effects=True, vmem_limit_bytes=56 * 1024 * 1024
        ),
    )(block_order, context_start[0], embed, *shaped, mod_weight)


def solution(mesh):
    placed = (
        P("stream", "frame", None),
        P("stream", "frame", None),
        P("stream", "frame", None),
        P("stream", "frame", None),
        P("stream", "frame", None),
        P("stream", None),
        P(),
        P(),
        P("stream", None),
    )
    return jax.shard_map(
        per_device, mesh=mesh, in_specs=placed, out_specs=P("frame", None), check_vma=False
    )
```

```python
import functools
import math

import jax
import jax.numpy as jnp
from jax import lax
from jax.experimental import pallas as pl
from jax.experimental.pallas import tpu as pltpu
from jax.sharding import PartitionSpec as P

HEAD_DIM = 128
HIDDEN = -1e30


def sinusoid(noise, emb_width):
    half_width = emb_width // 2
    frequency = jnp.exp(-math.log(10000.0) * jnp.arange(half_width, dtype=jnp.float32) / half_width)
    angles = 1000.0 * noise[..., None] * frequency
    return jnp.concatenate([jnp.cos(angles), jnp.sin(angles)], -1).astype(jnp.bfloat16)


def kernel(
    frames,
    streams,
    order_ref,
    start_ref,
    embed_ref,
    query_ref,
    key_ref,
    value_ref,
    latent_ref,
    target_ref,
    weight_ref,
    out_ref,
    query_in,
    key_in,
    value_in,
    diff_in,
    key_sorted,
    value_sorted,
    attn_all,
    latent_own,
    target_own,
    diff_own,
    weight_own,
    embed_all,
    sums_all,
    squares,
    base,
    partial,
    place,
    send_sems,
    recv_sems,
    side_send,
    side_recv,
    local_sems,
):
    me = lax.axis_index("frame")
    my_stream = lax.axis_index("stream")
    own, block_len, width = query_ref.shape
    local = width // frames
    blocks = diff_in.shape[0]
    groups = embed_ref.shape[0]
    per_group = blocks // groups
    group_len = per_group * block_len
    seq_len = blocks * block_len
    heads = local // HEAD_DIM

    barrier = pltpu.get_barrier_semaphore()

    @pl.loop(1, frames)
    def _(i):
        pl.semaphore_signal(barrier, inc=1, device_id={"frame": lax.rem(me + i, frames)})

    for i in range(1, streams):
        pl.semaphore_signal(
            barrier, inc=1, device_id={"stream": lax.rem(my_stream + i, streams)}
        )

    early = (
        pltpu.make_async_copy(latent_ref, latent_own, local_sems.at[0]),
        pltpu.make_async_copy(target_ref, target_own, local_sems.at[1]),
        pltpu.make_async_copy(
            weight_ref.at[pl.ds(me * local, local), :], weight_own, local_sems.at[2]
        ),
    )
    moved = ((key_ref, key_in), (query_ref, query_in), (value_ref, value_in))
    mine = tuple(
        pltpu.make_async_copy(
            source.at[:, :, pl.ds(pl.multiple_of(me * local + h * HEAD_DIM, HEAD_DIM), HEAD_DIM)],
            landing[h].at[pl.ds(me * own, own)],
            local_sems.at[4 + h * len(moved) + number],
        )
        for h in range(heads)
        for number, (source, landing) in enumerate(moved)
    )
    for copy in early + mine:
        copy.start()
    pl.semaphore_wait(barrier, frames - 1 + streams - 1)

    def remote(number, source, landing, offset, peer, slot):
        begin = pl.multiple_of(peer * local + offset, HEAD_DIM)
        return pltpu.make_async_remote_copy(
            src_ref=source.at[:, :, pl.ds(begin, landing.shape[2])],
            dst_ref=landing.at[pl.ds(slot * own, own)],
            send_sem=send_sems.at[number, peer],
            recv_sem=recv_sems.at[number, slot],
            device_id={"frame": peer},
        )

    def send_all(number, source, landing, offset):
        @pl.loop(1, frames)
        def _(i):
            peer = lax.rem(me + i, frames)
            remote(number, source, landing, offset, peer, me).start()

    def await_all(number, source, landing, offset):
        @pl.loop(1, frames)
        def _(i):
            peer = lax.rem(me + i, frames)
            remote(number, source, landing, offset, peer, peer).wait()

    last = heads * len(moved)
    for h in range(heads):
        for number, (source, landing) in enumerate(moved):
            send_all(h * len(moved) + number, source, landing[h], h * HEAD_DIM)

    def side_copies(part, source, landing):
        return [
            pltpu.make_async_remote_copy(
                src_ref=source,
                dst_ref=landing.at[my_stream],
                send_sem=side_send.at[part, i],
                recv_sem=side_recv.at[part, i],
                device_id={"stream": lax.rem(my_stream + i, streams)},
            )
            for i in range(1, streams)
        ]

    embed_copies = side_copies(0, embed_ref, embed_all)
    for copy in embed_copies:
        copy.start()
    embed_all[my_stream] = embed_ref[...]

    for copy in early:
        copy.wait()

    @pl.loop(0, frames)
    def _(i):
        columns = pl.ds(pl.multiple_of(i * local, local), local)
        for b in range(own):
            diff_own[b, :, columns] = (
                latent_own[b, :, columns].astype(jnp.float32)
                - target_own[b, :, columns].astype(jnp.float32)
            ).astype(jnp.bfloat16)

    my_diff = pltpu.make_async_copy(
        diff_own.at[:, :, pl.ds(me * local, local)],
        diff_in.at[pl.ds(me * own, own)],
        local_sems.at[3],
    )
    send_all(last, diff_own, diff_in, 0)
    my_diff.start()

    gate = lax.dot_general(
        embed_ref[...].astype(jnp.bfloat16),
        weight_own[...],
        (((1,), (1,)), ((), ())),
        preferred_element_type=jnp.float32,
    )

    @pl.loop(0, blocks)
    def _(t):
        found = jnp.int32(0)
        for b in range(blocks):
            found = jnp.where(order_ref[b] == t, b, found)
        place[t] = found

    for copy in mine:
        copy.wait()

    factor = math.log2(math.e) / math.sqrt(HEAD_DIM)
    ranges = math.gcd(groups, 4)
    for h in range(heads):
        lanes = slice(h * HEAD_DIM, (h + 1) * HEAD_DIM)
        for number, (source, landing) in enumerate(moved):
            await_all(h * len(moved) + number, source, landing[h], h * HEAD_DIM)

        @pl.loop(0, blocks)
        def _(t):
            rows = pl.ds(pl.multiple_of(t * block_len, block_len), block_len)
            key_sorted[rows, lanes] = key_in[h][place[t]]
            value_sorted[rows, lanes] = value_in[h][place[t]]

        for number in range(ranges):
            length = (number + 1) * (seq_len // ranges)

            @pl.loop(number * (groups // ranges), (number + 1) * (groups // ranges))
            def _(c):
                rows = jnp.concatenate(
                    [query_in[h][place[c * per_group + i]] for i in range(per_group)],
                    axis=0,
                )
                column_group = lax.broadcasted_iota(jnp.int32, (1, length), 1) // group_len
                bias = jnp.where(
                    (column_group >= start_ref[c]) & (column_group <= c), 0.0, HIDDEN
                ).astype(jnp.float32)
                scores = (
                    lax.dot_general(
                        rows,
                        key_sorted[:length, lanes],
                        (((1,), (1,)), ((), ())),
                        preferred_element_type=jnp.float32,
                    )
                    + bias
                )
                peak = jnp.max(scores, axis=-1, keepdims=True)
                unnorm = jnp.exp2((scores - peak) * factor)
                inverse = 1.0 / jnp.sum(unnorm, axis=-1, keepdims=True)
                probs = (unnorm * inverse).astype(jnp.bfloat16)
                attn = lax.dot_general(
                    probs,
                    value_sorted[:length, lanes],
                    (((1,), (0,)), ((), ())),
                    preferred_element_type=jnp.float32,
                ).astype(jnp.bfloat16)
                attn_all[pl.ds(c * per_group, per_group), :, lanes] = attn.reshape(
                    per_group, block_len, HEAD_DIM
                )
                wide = attn.astype(jnp.float32)
                squares[h, pl.ds(c, 1), :] = jnp.sum(wide * wide, axis=0, keepdims=True)

    base[...] = gate * jnp.concatenate([squares[h] for h in range(heads)], axis=1)

    def take(slot):
        for b in range(own):
            block = slot * own + b
            product = attn_all[order_ref[block]].astype(jnp.float32) * diff_in[block].astype(
                jnp.float32
            )
            partial[pl.ds(block, 1), :] = jnp.sum(product, axis=0, keepdims=True)

    my_diff.wait()
    take(me)

    @pl.loop(1, frames)
    def _(i):
        peer = lax.rem(me + frames - i, frames)
        remote(last, diff_own, diff_in, 0, peer, peer).wait_recv()
        take(peer)

    @pl.loop(0, groups)
    def _(c):
        total = base[pl.ds(c, 1), :]
        for i in range(per_group):
            total = total + partial[pl.ds(place[c * per_group + i], 1), :]
        sums_all[my_stream, pl.ds(c, 1), :] = total

    sum_copies = side_copies(1, sums_all.at[my_stream], sums_all)
    for copy in sum_copies:
        copy.start()
    for copy in embed_copies:
        copy.wait()
    for copy in sum_copies:
        copy.wait()

    @pl.loop(1, frames)
    def _(i):
        peer = lax.rem(me + i, frames)
        remote(last, diff_own, diff_in, 0, peer, me).wait_send()

    out_ref[...] = lax.dot_general(
        sums_all[...].reshape(streams * groups, local),
        embed_all[...].reshape(streams * groups, embed_ref.shape[1]),
        (((0,), (0,)), ((), ())),
        precision=lax.Precision.HIGHEST,
        preferred_element_type=jnp.float32,
    ) * (1.0 / math.sqrt(group_len))


def per_device(
    query, key, value, latent, target, noise_level, mod_weight, block_order, context_start
):
    frames = lax.axis_size("frame")
    streams = lax.axis_size("stream")
    tokens, width = query.shape[1:]
    local = width // frames
    blocks = block_order.shape[0]
    own = blocks // frames
    block_len = tokens // own
    groups = noise_level.shape[1]
    emb_width = mod_weight.shape[1]
    group_len = blocks // groups * block_len
    seq_len = blocks * block_len
    embed = sinusoid(noise_level[0], emb_width).astype(jnp.float32)
    bf16, f32 = jnp.bfloat16, jnp.float32
    shaped = [x.reshape(own, block_len, width) for x in (query, key, value, latent, target)]
    anywhere = pl.BlockSpec(memory_space=pl.ANY)
    scalars = pl.BlockSpec(memory_space=pltpu.SMEM)
    vectors = pl.BlockSpec(memory_space=pltpu.VMEM)
    heads = local // HEAD_DIM
    one_head = pltpu.VMEM((blocks, block_len, HEAD_DIM), bf16)
    landing = pltpu.VMEM((blocks, block_len, local), bf16)
    ordered = pltpu.VMEM((seq_len, local), bf16)
    held = pltpu.VMEM((own, block_len, width), bf16)
    return pl.pallas_call(
        functools.partial(kernel, frames, streams),
        out_shape=jax.ShapeDtypeStruct((local, emb_width), f32),
        in_specs=[scalars, scalars, vectors] + [anywhere] * 6,
        out_specs=vectors,
        scratch_shapes=[
            [one_head] * heads,
            [one_head] * heads,
            [one_head] * heads,
            landing,
            ordered,
            ordered,
            landing,
            held,
            held,
            held,
            pltpu.VMEM((local, emb_width), bf16),
            pltpu.VMEM((streams, groups, emb_width), f32),
            pltpu.VMEM((streams, groups, local), f32),
            pltpu.VMEM((heads, groups, HEAD_DIM), f32),
            pltpu.VMEM((groups, local), f32),
            pltpu.VMEM((blocks, local), f32),
            pltpu.SMEM((blocks,), jnp.int32),
            pltpu.SemaphoreType.DMA((3 * heads + 1, frames)),
            pltpu.SemaphoreType.DMA((3 * heads + 1, frames)),
            pltpu.SemaphoreType.DMA((2, streams)),
            pltpu.SemaphoreType.DMA((2, streams)),
            pltpu.SemaphoreType.DMA((4 + 3 * heads,)),
        ],
        compiler_params=pltpu.CompilerParams(
            collective_id=0, has_side_effects=True, vmem_limit_bytes=56 * 1024 * 1024
        ),
    )(block_order, context_start[0], embed, *shaped, mod_weight)


def solution(mesh):
    placed = (
        P("stream", "frame", None),
        P("stream", "frame", None),
        P("stream", "frame", None),
        P("stream", "frame", None),
        P("stream", "frame", None),
        P("stream", None),
        P(),
        P(),
        P("stream", None),
    )
    return jax.shard_map(
        per_device, mesh=mesh, in_specs=placed, out_specs=P("frame", None), check_vma=False
    )
```

```python
import functools
import math

import jax
import jax.numpy as jnp
from jax import lax
from jax.experimental import pallas as pl
from jax.experimental.pallas import tpu as pltpu
from jax.sharding import PartitionSpec as P

HEAD_DIM = 128
HIDDEN = -1e30


def kernel(
    frames,
    streams,
    order_ref,
    start_ref,
    noise_ref,
    frequency_ref,
    query_ref,
    key_ref,
    value_ref,
    latent_ref,
    target_ref,
    weight_ref,
    out_ref,
    query_in,
    key_in,
    value_in,
    diff_in,
    key_sorted,
    value_sorted,
    attn_all,
    latent_own,
    target_own,
    diff_own,
    weight_own,
    embed_all,
    sums_all,
    squares,
    base,
    partial,
    place,
    send_sems,
    recv_sems,
    side_send,
    side_recv,
    local_sems,
):
    me = lax.axis_index("frame")
    my_stream = lax.axis_index("stream")
    own, block_len, width = query_ref.shape
    local = width // frames
    blocks = diff_in.shape[0]
    groups = noise_ref.shape[0]
    per_group = blocks // groups
    group_len = per_group * block_len
    seq_len = blocks * block_len
    heads = local // HEAD_DIM

    barrier = pltpu.get_barrier_semaphore()

    @pl.loop(1, frames)
    def _(i):
        pl.semaphore_signal(barrier, inc=1, device_id={"frame": lax.rem(me + i, frames)})

    for i in range(1, streams):
        pl.semaphore_signal(
            barrier, inc=1, device_id={"stream": lax.rem(my_stream + i, streams)}
        )

    early = (
        pltpu.make_async_copy(latent_ref, latent_own, local_sems.at[0]),
        pltpu.make_async_copy(target_ref, target_own, local_sems.at[1]),
        pltpu.make_async_copy(
            weight_ref.at[pl.ds(me * local, local), :], weight_own, local_sems.at[2]
        ),
    )
    moved = ((key_ref, key_in), (query_ref, query_in), (value_ref, value_in))
    mine = tuple(
        pltpu.make_async_copy(
            source.at[:, :, pl.ds(pl.multiple_of(me * local + h * HEAD_DIM, HEAD_DIM), HEAD_DIM)],
            landing[h].at[pl.ds(me * own, own)],
            local_sems.at[4 + h * len(moved) + number],
        )
        for h in range(heads)
        for number, (source, landing) in enumerate(moved)
    )
    for copy in early + mine:
        copy.start()
    pl.semaphore_wait(barrier, frames - 1 + streams - 1)

    def remote(number, source, landing, offset, peer, slot):
        begin = pl.multiple_of(peer * local + offset, HEAD_DIM)
        return pltpu.make_async_remote_copy(
            src_ref=source.at[:, :, pl.ds(begin, landing.shape[2])],
            dst_ref=landing.at[pl.ds(slot * own, own)],
            send_sem=send_sems.at[number, peer],
            recv_sem=recv_sems.at[number, slot],
            device_id={"frame": peer},
        )

    def send_all(number, source, landing, offset):
        @pl.loop(1, frames)
        def _(i):
            peer = lax.rem(me + i, frames)
            remote(number, source, landing, offset, peer, me).start()

    def await_all(number, source, landing, offset):
        @pl.loop(1, frames)
        def _(i):
            peer = lax.rem(me + i, frames)
            remote(number, source, landing, offset, peer, peer).wait()

    last = heads * len(moved)
    for h in range(heads):
        for number, (source, landing) in enumerate(moved):
            send_all(h * len(moved) + number, source, landing[h], h * HEAD_DIM)

    def side_copies(part, source, landing):
        return [
            pltpu.make_async_remote_copy(
                src_ref=source,
                dst_ref=landing.at[my_stream],
                send_sem=side_send.at[part, i],
                recv_sem=side_recv.at[part, i],
                device_id={"stream": lax.rem(my_stream + i, streams)},
            )
            for i in range(1, streams)
        ]

    half_width = frequency_ref.shape[1]
    for c in range(groups):
        angles = (1000.0 * noise_ref[c]) * frequency_ref[...]
        waves = jnp.concatenate([jnp.cos(angles), jnp.sin(angles)], axis=1)
        embed_all[my_stream, c : c + 1, :] = waves.astype(jnp.bfloat16).astype(jnp.float32)

    for copy in early:
        copy.wait()

    @pl.loop(0, frames)
    def _(i):
        columns = pl.ds(pl.multiple_of(i * local, local), local)
        for b in range(own):
            diff_own[b, :, columns] = (
                latent_own[b, :, columns].astype(jnp.float32)
                - target_own[b, :, columns].astype(jnp.float32)
            ).astype(jnp.bfloat16)

    my_diff = pltpu.make_async_copy(
        diff_own.at[:, :, pl.ds(me * local, local)],
        diff_in.at[pl.ds(me * own, own)],
        local_sems.at[3],
    )
    send_all(last, diff_own, diff_in, 0)
    my_diff.start()

    gate = lax.dot_general(
        embed_all[my_stream].astype(jnp.bfloat16),
        weight_own[...],
        (((1,), (1,)), ((), ())),
        preferred_element_type=jnp.float32,
    )

    @pl.loop(0, blocks)
    def _(t):
        found = jnp.int32(0)
        for b in range(blocks):
            found = jnp.where(order_ref[b] == t, b, found)
        place[t] = found

    for copy in mine:
        copy.wait()

    factor = math.log2(math.e) / math.sqrt(HEAD_DIM)
    ranges = math.gcd(groups, 4)
    for h in range(heads):
        lanes = slice(h * HEAD_DIM, (h + 1) * HEAD_DIM)
        for number, (source, landing) in enumerate(moved):
            await_all(h * len(moved) + number, source, landing[h], h * HEAD_DIM)

        @pl.loop(0, blocks)
        def _(t):
            rows = pl.ds(pl.multiple_of(t * block_len, block_len), block_len)
            key_sorted[rows, lanes] = key_in[h][place[t]]
            value_sorted[rows, lanes] = value_in[h][place[t]]

        for number in range(ranges):
            length = (number + 1) * (seq_len // ranges)

            @pl.loop(number * (groups // ranges), (number + 1) * (groups // ranges))
            def _(c):
                rows = jnp.concatenate(
                    [query_in[h][place[c * per_group + i]] for i in range(per_group)],
                    axis=0,
                )
                column_group = lax.broadcasted_iota(jnp.int32, (1, length), 1) // group_len
                bias = jnp.where(
                    (column_group >= start_ref[c]) & (column_group <= c), 0.0, HIDDEN
                ).astype(jnp.float32)
                scores = (
                    lax.dot_general(
                        rows,
                        key_sorted[:length, lanes],
                        (((1,), (1,)), ((), ())),
                        preferred_element_type=jnp.float32,
                    )
                    + bias
                )
                peak = jnp.max(scores, axis=-1, keepdims=True)
                unnorm = jnp.exp2((scores - peak) * factor)
                inverse = 1.0 / jnp.sum(unnorm, axis=-1, keepdims=True)
                probs = (unnorm * inverse).astype(jnp.bfloat16)
                attn = lax.dot_general(
                    probs,
                    value_sorted[:length, lanes],
                    (((1,), (0,)), ((), ())),
                    preferred_element_type=jnp.float32,
                ).astype(jnp.bfloat16)
                attn_all[pl.ds(c * per_group, per_group), :, lanes] = attn.reshape(
                    per_group, block_len, HEAD_DIM
                )
                wide = attn.astype(jnp.float32)
                squares[h, pl.ds(c, 1), :] = jnp.sum(wide * wide, axis=0, keepdims=True)

    base[...] = gate * jnp.concatenate([squares[h] for h in range(heads)], axis=1)

    def take(slot):
        for b in range(own):
            block = slot * own + b
            product = attn_all[order_ref[block]].astype(jnp.float32) * diff_in[block].astype(
                jnp.float32
            )
            partial[pl.ds(block, 1), :] = jnp.sum(product, axis=0, keepdims=True)

    embed_copies = side_copies(0, embed_all.at[my_stream], embed_all)
    for copy in embed_copies:
        copy.start()
    my_diff.wait()
    take(me)

    @pl.loop(1, frames)
    def _(i):
        peer = lax.rem(me + frames - i, frames)
        remote(last, diff_own, diff_in, 0, peer, peer).wait_recv()
        take(peer)

    @pl.loop(0, groups)
    def _(c):
        total = base[pl.ds(c, 1), :]
        for i in range(per_group):
            total = total + partial[pl.ds(place[c * per_group + i], 1), :]
        sums_all[my_stream, pl.ds(c, 1), :] = total

    sum_copies = side_copies(1, sums_all.at[my_stream], sums_all)
    for copy in sum_copies:
        copy.start()
    for copy in embed_copies:
        copy.wait()
    for copy in sum_copies:
        copy.wait()

    @pl.loop(1, frames)
    def _(i):
        peer = lax.rem(me + i, frames)
        remote(last, diff_own, diff_in, 0, peer, me).wait_send()

    out_ref[...] = lax.dot_general(
        sums_all[...].reshape(streams * groups, local),
        embed_all[...].reshape(streams * groups, 2 * half_width),
        (((0,), (0,)), ((), ())),
        precision=lax.Precision.HIGHEST,
        preferred_element_type=jnp.float32,
    ) * (1.0 / math.sqrt(group_len))


def per_device(
    query, key, value, latent, target, noise_level, mod_weight, block_order, context_start
):
    frames = lax.axis_size("frame")
    streams = lax.axis_size("stream")
    tokens, width = query.shape[1:]
    local = width // frames
    blocks = block_order.shape[0]
    own = blocks // frames
    block_len = tokens // own
    groups = noise_level.shape[1]
    emb_width = mod_weight.shape[1]
    group_len = blocks // groups * block_len
    seq_len = blocks * block_len
    half_width = emb_width // 2
    exponents = jnp.arange(half_width, dtype=jnp.float32) / half_width
    frequency = jnp.exp(-math.log(10000.0) * exponents)[None, :]
    bf16, f32 = jnp.bfloat16, jnp.float32
    shaped = [x.reshape(own, block_len, width) for x in (query, key, value, latent, target)]
    anywhere = pl.BlockSpec(memory_space=pl.ANY)
    scalars = pl.BlockSpec(memory_space=pltpu.SMEM)
    vectors = pl.BlockSpec(memory_space=pltpu.VMEM)
    heads = local // HEAD_DIM
    one_head = pltpu.VMEM((blocks, block_len, HEAD_DIM), bf16)
    landing = pltpu.VMEM((blocks, block_len, local), bf16)
    ordered = pltpu.VMEM((seq_len, local), bf16)
    held = pltpu.VMEM((own, block_len, width), bf16)
    return pl.pallas_call(
        functools.partial(kernel, frames, streams),
        out_shape=jax.ShapeDtypeStruct((local, emb_width), f32),
        in_specs=[scalars, scalars, scalars, vectors] + [anywhere] * 6,
        out_specs=vectors,
        scratch_shapes=[
            [one_head] * heads,
            [one_head] * heads,
            [one_head] * heads,
            landing,
            ordered,
            ordered,
            landing,
            held,
            held,
            held,
            pltpu.VMEM((local, emb_width), bf16),
            pltpu.VMEM((streams, groups, emb_width), f32),
            pltpu.VMEM((streams, groups, local), f32),
            pltpu.VMEM((heads, groups, HEAD_DIM), f32),
            pltpu.VMEM((groups, local), f32),
            pltpu.VMEM((blocks, local), f32),
            pltpu.SMEM((blocks,), jnp.int32),
            pltpu.SemaphoreType.DMA((3 * heads + 1, frames)),
            pltpu.SemaphoreType.DMA((3 * heads + 1, frames)),
            pltpu.SemaphoreType.DMA((2, streams)),
            pltpu.SemaphoreType.DMA((2, streams)),
            pltpu.SemaphoreType.DMA((4 + 3 * heads,)),
        ],
        compiler_params=pltpu.CompilerParams(
            collective_id=0, has_side_effects=True, vmem_limit_bytes=56 * 1024 * 1024
        ),
    )(block_order, context_start[0], noise_level[0], frequency, *shaped, mod_weight)


def solution(mesh):
    placed = (
        P("stream", "frame", None),
        P("stream", "frame", None),
        P("stream", "frame", None),
        P("stream", "frame", None),
        P("stream", "frame", None),
        P("stream", None),
        P(),
        P(),
        P("stream", None),
    )
    return jax.shard_map(
        per_device, mesh=mesh, in_specs=placed, out_specs=P("frame", None), check_vma=False
    )
```
